32 devices in a mesh: lon: 8 (over y, x, core), lat: 4 (over z).
Axes of the slice: x: 2, y: 2, z: 4, core: 2. Of those that a mesh axis runs over, the one named last changes fastest.
Arguments:
- fields: bfloat16 [32, 256, 256], P('lat', 'lon'), may hold values from -6 to 6
- norm_lon: float32 [256], replicated, may hold values from 0.25 to 1.75
- query_lon: bfloat16 [256, 256], replicated, may hold values from -0.375 to 0.375
- key_lon: bfloat16 [256, 256], replicated, may hold values from -0.375 to 0.375
- value_lon: bfloat16 [256, 256], replicated, may hold values from -0.375 to 0.375
- out_lon: bfloat16 [256, 256], replicated, may hold values from -0.375 to 0.375
- temp_lon: float32 [8], replicated, may hold values from 0.5 to 12
- bias_lon: float32 [8], replicated, may hold values from -2 to 2
- norm_lat: float32 [256], replicated, may hold values from 0.25 to 1.75
- query_lat: bfloat16 [256, 256], replicated, may hold values from -0.375 to 0.375
- key_lat: bfloat16 [256, 256], replicated, may hold values from -0.375 to 0.375
- value_lat: bfloat16 [256, 256], replicated, may hold values from -0.375 to 0.375
- out_lat: bfloat16 [256, 256], replicated, may hold values from -0.375 to 0.375
- temp_lat: float32 [8], replicated, may hold values from 0.5 to 12
- bias_lat: float32 [8], replicated, may hold values from -4 to 0
- norm_mlp: float32 [256], replicated, may hold values from 0.25 to 1.75
- w_gate: bfloat16 [256, 1024], replicated, may hold values from -0.375 to 0.375
- w_up: bfloat16 [256, 1024], replicated, may hold values from -0.375 to 0.375
- w_down: bfloat16 [1024, 256], replicated, may hold values from -0.1875 to 0.1875
Outputs:
- updated: bfloat16 [32, 256, 256], P('lat', 'lon')
The draws below stay inside these ranges and needn't reach their ends.
All inputs are finite; a program needn't handle non-finite values.
Results may differ from the reference program's by a relative error of at most 0.018.
The reference program's roundings to bfloat16 on the way count: a program that leaves them out, or rounds other values in their place, can miss the bound.
Values may be sent and summed in bfloat16 or wider, within the bound.
A program may use at most 64 MiB of HBM per device.

```python
import math
import jax
import jax.numpy as jnp
from jax import lax

D = 256
HEADS = 8
FF = 1024
HEAD = 32
LON_DEV = 32
NLON = 256
NLAT = 32


def block_scale(rng, shape, cuts, least, high):
    def one(dim, parts):
        steps = jax.random.uniform(jax.random.fold_in(jax.random.fold_in(rng, 6), dim), (parts,), jnp.float32, least / len(cuts), high / len(cuts))
        return jnp.repeat(jnp.exp(steps), shape[dim] // parts).reshape((-1,) + (1,) * (len(shape) - dim - 1))

    loudness = one(*cuts[0])
    for cut in cuts[1:]:
        loudness = loudness * one(*cut)
    return loudness


def scatter_about(own_key, extent, scale, reach, shards=(), kind=jnp.bfloat16):
    entries = jax.random.normal(own_key, extent, jnp.float32) * scale
    if len(shards) > 0:
        entries = block_scale(own_key, extent, shards, -0.22, 0.18) * entries
    return jnp.clip(entries, min=-reach, max=reach).astype(kind)


def setup_inputs(seed: int = 0) -> dict:
    seeds = jax.random.split(jax.random.key(seed), 20)
    fields = scatter_about(seeds[0], (NLAT, NLON, D), 1.0, 6.0, ((0, 4), (1, 8)))
    norm_lon = jnp.clip(1.0 + 0.15 * jax.random.normal(seeds[1], (D,), jnp.float32), 0.25, 1.75)
    query_lon = scatter_about(seeds[2], (D, D), D ** -0.5, 0.375)
    key_lon = scatter_about(seeds[3], (D, D), D ** -0.5, 0.375)
    value_lon = scatter_about(seeds[4], (D, D), D ** -0.5, 0.375)
    out_lon = scatter_about(seeds[5], (D, D), D ** -0.5, 0.375)
    temp_lon = jnp.clip(jnp.exp(jax.random.uniform(seeds[6], (HEADS,), jnp.float32, math.log(0.5), math.log(12.0))), 0.5, 12.0)
    bias_lon = jnp.clip(jax.random.uniform(seeds[7], (HEADS,), jnp.float32, -2.0, 2.0), -2.0, 2.0)
    norm_lat = jnp.clip(1.0 + 0.15 * jax.random.normal(seeds[8], (D,), jnp.float32), 0.25, 1.75)
    query_lat = scatter_about(seeds[9], (D, D), D ** -0.5, 0.375)
    key_lat = scatter_about(seeds[10], (D, D), D ** -0.5, 0.375)
    value_lat = scatter_about(seeds[11], (D, D), D ** -0.5, 0.375)
    out_lat = scatter_about(seeds[12], (D, D), D ** -0.5, 0.375)
    temp_lat = jnp.clip(jnp.exp(jax.random.uniform(seeds[13], (HEADS,), jnp.float32, math.log(0.5), math.log(12.0))), 0.5, 12.0)
    bias_lat = jnp.clip(jax.random.uniform(seeds[14], (HEADS,), jnp.float32, -4.0, 0.0), -4.0, 0.0)
    norm_mlp = jnp.clip(1.0 + 0.15 * jax.random.normal(seeds[15], (D,), jnp.float32), 0.25, 1.75)
    w_gate = scatter_about(seeds[16], (D, FF), D ** -0.5, 0.375)
    w_up = scatter_about(seeds[17], (D, FF), D ** -0.5, 0.375)
    w_down = scatter_about(seeds[18], (FF, D), FF ** -0.5, 0.1875)
    return dict(fields=fields, norm_lon=norm_lon, query_lon=query_lon, key_lon=key_lon, value_lon=value_lon, out_lon=out_lon, temp_lon=temp_lon, bias_lon=bias_lon, norm_lat=norm_lat, query_lat=query_lat, key_lat=key_lat, value_lat=value_lat, out_lat=out_lat, temp_lat=temp_lat, bias_lat=bias_lat, norm_mlp=norm_mlp, w_gate=w_gate, w_up=w_up, w_down=w_down)


def normalize(values, gain):
    wide = values.astype(jnp.float32)
    factor = lax.rsqrt(lax.optimization_barrier(jnp.mean(wide * wide, axis=-1, keepdims=True)) + 1e-06)
    return (wide * factor * gain).astype(jnp.bfloat16)

def project(values, weight):
    return jnp.dot(values, weight, preferred_element_type=jnp.float32).astype(jnp.bfloat16)

def attend_lat(queries, keys, values, temp, bias):
    count, cols, depth = queries.shape
    heads = temp.shape[0]
    size = depth // heads
    qh = queries.reshape(count, cols, heads, size).astype(jnp.float32)
    kh = keys.reshape(count, cols, heads, size).astype(jnp.float32)
    vh = values.reshape(count, cols, heads, size).astype(jnp.float32)
    scores = jnp.einsum('ichd,jchd->chij', qh, kh)
    place = jnp.arange(count, dtype=jnp.int32)
    spread = jnp.abs(place[:, None] - place[None, :]).astype(jnp.float32) / count
    scores = scores * (temp / math.sqrt(size))[None, :, None, None] + bias[None, :, None, None] * spread[None, None]
    expo = jnp.exp(scores - lax.optimization_barrier(jnp.max(scores, axis=-1, keepdims=True)))
    denom = lax.optimization_barrier(jnp.sum(expo, axis=-1))
    mixed = jnp.einsum('chij,jchd->ichd', expo.astype(jnp.bfloat16).astype(jnp.float32), vh)
    mixed = mixed / jnp.transpose(denom, (2, 0, 1))[..., None]
    return mixed.astype(jnp.bfloat16).reshape(count, cols, depth)

def reference(fields, norm_lon, query_lon, key_lon, value_lon, out_lon, temp_lon, bias_lon, norm_lat, query_lat, key_lat, value_lat, out_lat, temp_lat, bias_lat, norm_mlp, w_gate, w_up, w_down):
    resid = fields.astype(jnp.float32)
    normed = normalize(resid, norm_lon)
    queries = project(normed, query_lon)
    keys = project(normed, key_lon)
    values = project(normed, value_lon)
    place = jnp.arange(NLON, dtype=jnp.int32)
    angle = (place[:, None] - place[None, :]).astype(jnp.float32) * (2.0 * math.pi / NLON)
    wave = jnp.cos(angle)

    def lon_row(items):
        qr, kr, vr = items
        qh = qr.reshape(NLON, HEADS, HEAD).astype(jnp.float32)
        kh = kr.reshape(NLON, HEADS, HEAD).astype(jnp.float32)
        vh = vr.reshape(NLON, HEADS, HEAD).astype(jnp.float32)
        scores = jnp.einsum('ihd,jhd->hij', qh, kh)
        scores = scores * (temp_lon / math.sqrt(HEAD))[:, None, None] + bias_lon[:, None, None] * wave[None]
        expo = jnp.exp(scores - lax.optimization_barrier(jnp.max(scores, axis=-1, keepdims=True)))
        denom = lax.optimization_barrier(jnp.sum(expo, axis=-1))
        mixed = jnp.einsum('hij,jhd->ihd', expo.astype(jnp.bfloat16).astype(jnp.float32), vh)
        mixed = mixed / jnp.transpose(denom)[..., None]
        return mixed.astype(jnp.bfloat16).reshape(NLON, D)
    attended = lax.map(lon_row, (queries, keys, values))
    first = resid + jnp.dot(attended, out_lon, preferred_element_type=jnp.float32)
    normed_lat = normalize(first, norm_lat)
    blocks = NLON // LON_DEV

    def split(values_in):
        return jnp.transpose(values_in.reshape(NLAT, blocks, LON_DEV, D), (1, 0, 2, 3))
    q2 = split(project(normed_lat, query_lat))
    k2 = split(project(normed_lat, key_lat))
    v2 = split(project(normed_lat, value_lat))
    mixed_lat = lax.map(lambda items: attend_lat(items[0], items[1], items[2], temp_lat, bias_lat), (q2, k2, v2))
    mixed_lat = jnp.transpose(mixed_lat, (1, 0, 2, 3)).reshape(NLAT, NLON, D)
    second = first + jnp.dot(mixed_lat, out_lat, preferred_element_type=jnp.float32)
    normed_mlp = normalize(second, norm_mlp)
    gate = jnp.dot(normed_mlp, w_gate, preferred_element_type=jnp.float32)
    upper = jnp.dot(normed_mlp, w_up, preferred_element_type=jnp.float32)
    hidden = (jax.nn.silu(gate) * upper).astype(jnp.bfloat16)
    return (second + jnp.dot(hidden, w_down, preferred_element_type=jnp.float32)).astype(jnp.bfloat16)
```

```python
import math

import jax
import jax.numpy as jnp
import functools
import numpy as np
from jax import lax
from jax.experimental import pallas as pl
from jax.experimental.pallas import tpu as pltpu
from jax.sharding import PartitionSpec as P


def normalize(values, gain):
    factor = lax.rsqrt(jnp.mean(values * values, axis=-1, keepdims=True) + 1e-06)
    return (values * factor * gain).astype(jnp.bfloat16)


def project(values, weight):
    return jnp.dot(values, weight, preferred_element_type=jnp.float32).astype(jnp.bfloat16)


def attend_lat(queries, keys, values, temp, bias):
    count, cols, depth = queries.shape
    heads = temp.shape[0]
    size = depth // heads
    qh = queries.reshape(count, cols, heads, size)
    kh = keys.reshape(count, cols, heads, size)
    vh = values.reshape(count, cols, heads, size)
    scores = jnp.einsum("ichd,jchd->chij", qh, kh, preferred_element_type=jnp.float32)
    place = jnp.arange(count, dtype=jnp.int32)
    spread = jnp.abs(place[:, None] - place[None, :]).astype(jnp.float32) / count
    scores = (
        scores * (temp / math.sqrt(size))[None, :, None, None]
        + bias[None, :, None, None] * spread[None, None]
    )
    expo = jnp.exp(scores - jnp.max(scores, axis=-1, keepdims=True))
    denom = jnp.sum(expo, axis=-1)
    mixed = jnp.einsum(
        "chij,jchd->ichd", expo.astype(jnp.bfloat16), vh, preferred_element_type=jnp.float32
    )
    mixed = mixed / jnp.transpose(denom, (2, 0, 1))[..., None]
    return mixed.astype(jnp.bfloat16).reshape(count, cols, depth)


def body(
    fields,
    norm_lon,
    query_lon,
    key_lon,
    value_lon,
    out_lon,
    temp_lon,
    bias_lon,
    norm_lat,
    query_lat,
    key_lat,
    value_lat,
    out_lat,
    temp_lat,
    bias_lat,
    norm_mlp,
    w_gate,
    w_up,
    w_down,
):
    rows, width, depth = fields.shape
    heads = temp_lon.shape[0]
    size = depth // heads
    total_lon = width * lax.axis_size("lon")
    resid = fields.astype(jnp.float32)
    normed = normalize(resid, norm_lon)
    scale_lon = temp_lon / math.sqrt(size)
    query_place = lax.axis_index("lon") * width + jnp.arange(width, dtype=jnp.int32)
    queries = project(normed, query_lon).reshape(rows, width, heads, size)
    piece = lax.all_gather(normed, "lon", axis=1, tiled=True)
    keys = project(piece, key_lon)
    count = keys.shape[1]
    key_place = jnp.arange(count, dtype=jnp.int32)
    angle = (query_place[:, None] - key_place[None, :]).astype(jnp.float32) * (
        2.0 * math.pi / total_lon
    )
    wave = jnp.cos(angle)

    def one_row(items):
        query_row, key_row, value_row, peak, total, accum = items
        key_heads = key_row.reshape(count, heads, size)
        value_heads = value_row.reshape(count, heads, size)
        scores = jnp.einsum(
            "ihd,jhd->hij", query_row, key_heads, preferred_element_type=jnp.float32
        )
        scores = scores * scale_lon[:, None, None] + bias_lon[:, None, None] * wave[None]
        fresh = jnp.maximum(peak, jnp.max(scores, axis=-1))
        shrink = jnp.exp(peak - fresh)
        expo = jnp.exp(scores - fresh[..., None])
        total = total * shrink + jnp.sum(expo, axis=-1)
        mixed = jnp.einsum(
            "hij,jhd->ihd",
            expo.astype(jnp.bfloat16),
            value_heads,
            preferred_element_type=jnp.float32,
        )
        accum = accum.reshape(width, heads, size) * jnp.transpose(shrink)[:, :, None] + mixed
        return (fresh, total, accum.reshape(width, depth))

    peak = jnp.full((rows, heads, width), -1e30, jnp.float32)
    total = jnp.zeros((rows, heads, width), jnp.float32)
    accum = jnp.zeros((rows, width, depth), jnp.float32)
    peak, total, accum = lax.map(
        one_row, (queries, keys, project(piece, value_lon), peak, total, accum)
    )
    attended = accum.reshape(rows, width, heads, size) / jnp.transpose(total, (0, 2, 1))[..., None]
    attended = attended.astype(jnp.bfloat16).reshape(rows, width, depth)
    first = resid + jnp.dot(attended, out_lon, preferred_element_type=jnp.float32)
    normed_lat = normalize(first, norm_lat)
    query_col = project(normed_lat, query_lat)
    key_col = project(normed_lat, key_lat)
    value_col = project(normed_lat, value_lat)
    query_col, key_col, value_col = (
        lax.all_to_all(query_col, "lat", split_axis=1, concat_axis=0, tiled=True),
        lax.all_to_all(key_col, "lat", split_axis=1, concat_axis=0, tiled=True),
        lax.all_to_all(value_col, "lat", split_axis=1, concat_axis=0, tiled=True),
    )
    mixed_lat = attend_lat(query_col, key_col, value_col, temp_lat, bias_lat)
    returned = lax.all_to_all(mixed_lat, "lat", split_axis=0, concat_axis=1, tiled=True)
    second = first + jnp.dot(returned, out_lat, preferred_element_type=jnp.float32)
    normed_mlp = normalize(second, norm_mlp)
    gate = jnp.dot(normed_mlp, w_gate, preferred_element_type=jnp.float32)
    upper = jnp.dot(normed_mlp, w_up, preferred_element_type=jnp.float32)
    hidden = (jax.nn.silu(gate) * upper).astype(jnp.bfloat16)
    return (second + jnp.dot(hidden, w_down, preferred_element_type=jnp.float32)).astype(
        jnp.bfloat16
    )


NT = (((1,), (1,)), ((), ()))
MESH = pl.DeviceIdType.MESH
F32 = jnp.float32
BF16 = jnp.bfloat16


def mm(a, b):
    return jnp.dot(a, b, preferred_element_type=F32)


def mm_nt(a, b):
    return lax.dot_general(a, b, NT, preferred_element_type=F32)


def iota(shape, dim):
    return lax.broadcasted_iota(jnp.int32, shape, dim)


def heads_t(keys, queries_t, values_t, temp, bias, table, mask, heads, size):
    outs = []
    for h in range(heads):
        part = slice(h * size, (h + 1) * size)
        scores = mm(keys[:, part], queries_t[part, :])
        scores = scores * (temp[h] / math.sqrt(size)) + bias[h] * table
        if mask is not None:
            scores = scores + mask
        expo = jnp.exp(scores - jnp.max(scores, axis=0, keepdims=True))
        denom = jnp.sum(expo, axis=0, keepdims=True)
        outs.append(mm(values_t[part, :], expo.astype(BF16)) / denom)
    return jnp.concatenate(outs, axis=0).astype(BF16)


def block_kernel(
    n_lon, n_lat, rows, width, depth, heads,
    fields, gain_lon, gain_lat, gain_mlp, temp_lon, bias_lon, temp_lat, bias_lat,
    wave_h, wq1_h, wk1_h, wv1_h, wo1_h, wq2_h, wk2_h, wv2_h, wo2_h, wg_h, wu_h, wd_h,
    out,
    wave, wq1, wk1, wv1, wo1, wq2, wk2, wv2, wo2, wg, wu, wd,
    norm_out, norm_in, field_out, field_in, att_out, att_in, upd_out,
    local_sem, s1, r1, s2, r2, s3, r3, s4, r4,
):
    me_lon = lax.axis_index("lon")
    me_lat = lax.axis_index("lat")
    total = n_lon * n_lat
    me = me_lon * n_lat + me_lat
    size = depth // heads
    cols = width // n_lat
    count = n_lat * rows
    cells = rows * width

    loads = [
        pltpu.make_async_copy(src, dst, local_sem.at[i])
        for i, (src, dst) in enumerate(
            [(wq1_h, wq1), (wk1_h, wk1), (wv1_h, wv1), (wave_h, wave), (wo1_h, wo1), (wq2_h, wq2),
             (wk2_h, wk2), (wv2_h, wv2), (wo2_h, wo2), (wg_h, wg), (wu_h, wu), (wd_h, wd)]
        )
    ]
    for load in loads:
        load.start()

    barrier = pltpu.get_barrier_semaphore()

    def greet(step, carry):
        peer = lax.rem(me + step, total)
        pl.semaphore_signal(
            barrier, inc=1, device_id=(peer // n_lat, lax.rem(peer, n_lat)), device_id_type=MESH
        )
        return carry

    lax.fori_loop(1, total, greet, 0)

    wide = fields[...].astype(F32)
    norm_out[...] = normalize(wide, gain_lon[...][None])
    pieces = wide.reshape(rows, n_lat, cols, depth).astype(BF16)
    for a in range(n_lat):
        field_out[a] = pieces[:, a]

    pl.semaphore_wait(barrier, total - 1)

    def send_norm(step):
        peer = lax.rem(me_lon + step, n_lon)
        return pltpu.make_async_remote_copy(
            src_ref=norm_out.at[peer], dst_ref=norm_in.at[me_lon], send_sem=s1.at[step],
            recv_sem=r1.at[step], device_id=(peer, me_lat), device_id_type=MESH,
        )

    def lat_copy(step, src, dst, ssem, rsem):
        peer = lax.rem(me_lat + step, n_lat)
        return pltpu.make_async_remote_copy(
            src_ref=src.at[peer], dst_ref=dst.at[me_lat], send_sem=ssem.at[step],
            recv_sem=rsem.at[step], device_id=(me_lon, peer), device_id_type=MESH,
        )

    sends1 = [send_norm(step) for step in range(1, n_lon)]
    for copy in sends1:
        copy.start()
    sends2 = [lat_copy(step, field_out, field_in, s2, r2) for step in range(1, n_lat)]
    for copy in sends2:
        copy.start()
    norm_in[pl.ds(me_lon, 1)] = norm_out[pl.ds(me_lon, 1)]
    field_in[pl.ds(me_lat, 1)] = field_out[pl.ds(me_lat, 1)]

    shape = (cells, cells)
    lanes = iota(shape, 1)
    subs = iota(shape, 0)
    to_cols = (lax.rem(subs, count) * cols + subs // count == lanes).astype(F32).astype(BF16)
    from_cols = (lax.rem(lanes, count) * cols + lanes // count == subs).astype(F32).astype(BF16)
    eye = (lanes == subs).astype(F32).astype(BF16)
    half = cells // 2
    hs, hl = iota((half, half), 0), iota((half, half), 1)
    spread = jnp.abs(lax.rem(hs, count) - lax.rem(hl, count)).astype(F32) / count
    mask = jnp.where(hs // count == hl // count, 0.0, -1e30).astype(F32)

    for load in loads[:4]:
        load.wait()
    wq_t = wq1[...].T
    wv_t = wv1[...].T

    for copy in sends1:
        copy.wait_recv()

    nlon = n_lon * width
    normed = norm_in[...].reshape(nlon, depth)
    keys = mm(normed, wk1[...]).astype(BF16)
    queries_t = mm_nt(wq_t, normed).astype(BF16)
    values_t = mm_nt(wv_t, normed).astype(BF16)
    att_t = heads_t(keys, queries_t, values_t, temp_lon, bias_lon, wave[...], None, heads, size)
    att = mm_nt(eye, att_t)
    att_out[...] = att.reshape(total, cols, depth).astype(BF16)

    my_row = me_lat * rows + me_lon

    def att_copy(step):
        peer = lax.rem(me + step, total)
        return pltpu.make_async_remote_copy(
            src_ref=att_out.at[peer], dst_ref=att_in.at[my_row], send_sem=s3.at[step],
            recv_sem=r3.at[step], device_id=(peer // n_lat, lax.rem(peer, n_lat)),
            device_id_type=MESH,
        )

    def start_att(step, carry):
        att_copy(step).start()
        return carry

    def wait_att(step, carry):
        att_copy(step).wait_recv()
        return carry

    def wait_att_send(step, carry):
        att_copy(step).wait_send()
        return carry

    lax.fori_loop(1, total, start_att, 0)
    att_in[pl.ds(my_row, 1)] = att_out[pl.ds(me, 1)]

    for load in loads[4:]:
        load.wait()
    wq2_t = wq2[...].T
    wv2_t = wv2[...].T
    for copy in sends2:
        copy.wait_recv()
    lax.fori_loop(1, total, wait_att, 0)

    resid = field_in[...].astype(F32).reshape(cells, depth)
    attended = att_in[...].astype(F32).reshape(cells, depth).astype(BF16)
    first = resid + mm(attended, wo1[...])
    normed = mm(to_cols, normalize(first, gain_lat[...])).astype(BF16)
    keys = mm(normed, wk2[...]).astype(BF16)
    queries_t = mm_nt(wq2_t, normed).astype(BF16)
    values_t = mm_nt(wv2_t, normed).astype(BF16)
    parts = []
    for part in (slice(0, half), slice(half, cells)):
        parts.append(
            heads_t(keys[part], queries_t[:, part], values_t[:, part], temp_lat, bias_lat,
                    spread, mask, heads, size)
        )
    att_t = jnp.concatenate(parts, axis=1)
    attended = mm_nt(from_cols, att_t).astype(BF16)
    second = first + mm(attended, wo2[...])
    normed = normalize(second, gain_mlp[...])
    ff = wg.shape[1]
    step_ff = min(ff, 256)
    for f in range(0, ff, step_ff):
        gate = mm(normed, wg[:, f:f + step_ff])
        upper = mm(normed, wu[:, f:f + step_ff])
        hidden = (gate / (1.0 + jnp.exp(-gate)) * upper).astype(BF16)
        second = second + mm(hidden, wd[f:f + step_ff, :])
    upd_out[...] = second.reshape(n_lat, rows, cols, depth).astype(BF16)

    sends4 = [lat_copy(step, upd_out, out, s4, r4) for step in range(1, n_lat)]
    for copy in sends4:
        copy.start()
    out[pl.ds(me_lat, 1)] = upd_out[pl.ds(me_lat, 1)]
    for copy in sends1:
        copy.wait_send()
    for copy in sends2:
        copy.wait_send()
    lax.fori_loop(1, total, wait_att_send, 0)
    for copy in sends4:
        copy.wait()


def fused_body(
    fields, norm_lon, query_lon, key_lon, value_lon, out_lon, temp_lon, bias_lon,
    norm_lat, query_lat, key_lat, value_lat, out_lat, temp_lat, bias_lat,
    norm_mlp, w_gate, w_up, w_down,
):
    rows, width, depth = fields.shape
    heads = temp_lon.shape[0]
    n_lon, n_lat = lax.axis_size("lon"), lax.axis_size("lat")
    cols = width // n_lat
    nlon = width * n_lon
    total = n_lon * n_lat
    place = np.arange(nlon)
    wave = np.cos((place[:, None] - place[None, :]) * (2.0 * math.pi / nlon)).astype(np.float32)
    vmem = pl.BlockSpec(memory_space=pltpu.VMEM)
    smem = pl.BlockSpec(memory_space=pltpu.SMEM)
    hbm = pl.BlockSpec(memory_space=pl.ANY)
    weights = (query_lon, key_lon, value_lon, out_lon, query_lat, key_lat, value_lat, out_lat,
               w_gate, w_up, w_down)
    dma = pltpu.SemaphoreType.DMA
    updated = pl.pallas_call(
        functools.partial(block_kernel, n_lon, n_lat, rows, width, depth, heads),
        out_shape=jax.ShapeDtypeStruct((n_lat, rows, cols, depth), BF16),
        in_specs=[vmem] * 4 + [smem] * 4 + [hbm] * 12,
        out_specs=vmem,
        scratch_shapes=[pltpu.VMEM((nlon, nlon), F32)]
        + [pltpu.VMEM(w.shape, w.dtype) for w in weights]
        + [
            pltpu.VMEM((rows, width, depth), BF16),
            pltpu.VMEM((n_lon, width, depth), BF16),
            pltpu.VMEM((n_lat, rows, cols, depth), BF16),
            pltpu.VMEM((n_lat, rows, cols, depth), BF16),
            pltpu.VMEM((total, cols, depth), BF16),
            pltpu.VMEM((n_lat * rows, cols, depth), BF16),
            pltpu.VMEM((n_lat, rows, cols, depth), BF16),
            dma((12,)),
            dma((n_lon,)), dma((n_lon,)),
            dma((n_lat,)), dma((n_lat,)),
            dma((total,)), dma((total,)),
            dma((n_lat,)), dma((n_lat,)),
        ],
        compiler_params=pltpu.CompilerParams(collective_id=0, has_side_effects=True),
    )(
        fields, norm_lon[None], norm_lat[None], norm_mlp[None], temp_lon, bias_lon, temp_lat, bias_lat,
        jnp.asarray(wave), *weights,
    )
    return jnp.transpose(updated, (1, 0, 2, 3)).reshape(rows, width, depth)


def choose(*args):
    rows, width, _ = args[0].shape
    n_lon, n_lat = lax.axis_size("lon"), lax.axis_size("lat")
    if rows == n_lon and width % n_lat == 0 and width // n_lat == 8:
        return fused_body(*args)
    return body(*args)


def solution(mesh):
    in_specs = (P("lat", "lon", None),) + (P(),) * 18
    out_specs = P("lat", "lon", None)
    return jax.shard_map(choose, mesh=mesh, in_specs=in_specs, out_specs=out_specs, check_vma=False)
```

```python
import math

import jax
import jax.numpy as jnp
import functools
import numpy as np
from jax import lax
from jax.experimental import pallas as pl
from jax.experimental.pallas import tpu as pltpu
from jax.sharding import PartitionSpec as P


def normalize(values, gain):
    factor = lax.rsqrt(jnp.mean(values * values, axis=-1, keepdims=True) + 1e-06)
    return (values * factor * gain).astype(jnp.bfloat16)


def project(values, weight):
    return jnp.dot(values, weight, preferred_element_type=jnp.float32).astype(jnp.bfloat16)


def attend_lat(queries, keys, values, temp, bias):
    count, cols, depth = queries.shape
    heads = temp.shape[0]
    size = depth // heads
    qh = queries.reshape(count, cols, heads, size)
    kh = keys.reshape(count, cols, heads, size)
    vh = values.reshape(count, cols, heads, size)
    scores = jnp.einsum("ichd,jchd->chij", qh, kh, preferred_element_type=jnp.float32)
    place = jnp.arange(count, dtype=jnp.int32)
    spread = jnp.abs(place[:, None] - place[None, :]).astype(jnp.float32) / count
    scores = (
        scores * (temp / math.sqrt(size))[None, :, None, None]
        + bias[None, :, None, None] * spread[None, None]
    )
    expo = jnp.exp(scores - jnp.max(scores, axis=-1, keepdims=True))
    denom = jnp.sum(expo, axis=-1)
    mixed = jnp.einsum(
        "chij,jchd->ichd", expo.astype(jnp.bfloat16), vh, preferred_element_type=jnp.float32
    )
    mixed = mixed / jnp.transpose(denom, (2, 0, 1))[..., None]
    return mixed.astype(jnp.bfloat16).reshape(count, cols, depth)


def body(
    fields,
    norm_lon,
    query_lon,
    key_lon,
    value_lon,
    out_lon,
    temp_lon,
    bias_lon,
    norm_lat,
    query_lat,
    key_lat,
    value_lat,
    out_lat,
    temp_lat,
    bias_lat,
    norm_mlp,
    w_gate,
    w_up,
    w_down,
):
    rows, width, depth = fields.shape
    heads = temp_lon.shape[0]
    size = depth // heads
    total_lon = width * lax.axis_size("lon")
    resid = fields.astype(jnp.float32)
    normed = normalize(resid, norm_lon)
    scale_lon = temp_lon / math.sqrt(size)
    query_place = lax.axis_index("lon") * width + jnp.arange(width, dtype=jnp.int32)
    queries = project(normed, query_lon).reshape(rows, width, heads, size)
    piece = lax.all_gather(normed, "lon", axis=1, tiled=True)
    keys = project(piece, key_lon)
    count = keys.shape[1]
    key_place = jnp.arange(count, dtype=jnp.int32)
    angle = (query_place[:, None] - key_place[None, :]).astype(jnp.float32) * (
        2.0 * math.pi / total_lon
    )
    wave = jnp.cos(angle)

    def one_row(items):
        query_row, key_row, value_row, peak, total, accum = items
        key_heads = key_row.reshape(count, heads, size)
        value_heads = value_row.reshape(count, heads, size)
        scores = jnp.einsum(
            "ihd,jhd->hij", query_row, key_heads, preferred_element_type=jnp.float32
        )
        scores = scores * scale_lon[:, None, None] + bias_lon[:, None, None] * wave[None]
        fresh = jnp.maximum(peak, jnp.max(scores, axis=-1))
        shrink = jnp.exp(peak - fresh)
        expo = jnp.exp(scores - fresh[..., None])
        total = total * shrink + jnp.sum(expo, axis=-1)
        mixed = jnp.einsum(
            "hij,jhd->ihd",
            expo.astype(jnp.bfloat16),
            value_heads,
            preferred_element_type=jnp.float32,
        )
        accum = accum.reshape(width, heads, size) * jnp.transpose(shrink)[:, :, None] + mixed
        return (fresh, total, accum.reshape(width, depth))

    peak = jnp.full((rows, heads, width), -1e30, jnp.float32)
    total = jnp.zeros((rows, heads, width), jnp.float32)
    accum = jnp.zeros((rows, width, depth), jnp.float32)
    peak, total, accum = lax.map(
        one_row, (queries, keys, project(piece, value_lon), peak, total, accum)
    )
    attended = accum.reshape(rows, width, heads, size) / jnp.transpose(total, (0, 2, 1))[..., None]
    attended = attended.astype(jnp.bfloat16).reshape(rows, width, depth)
    first = resid + jnp.dot(attended, out_lon, preferred_element_type=jnp.float32)
    normed_lat = normalize(first, norm_lat)
    query_col = project(normed_lat, query_lat)
    key_col = project(normed_lat, key_lat)
    value_col = project(normed_lat, value_lat)
    query_col, key_col, value_col = (
        lax.all_to_all(query_col, "lat", split_axis=1, concat_axis=0, tiled=True),
        lax.all_to_all(key_col, "lat", split_axis=1, concat_axis=0, tiled=True),
        lax.all_to_all(value_col, "lat", split_axis=1, concat_axis=0, tiled=True),
    )
    mixed_lat = attend_lat(query_col, key_col, value_col, temp_lat, bias_lat)
    returned = lax.all_to_all(mixed_lat, "lat", split_axis=0, concat_axis=1, tiled=True)
    second = first + jnp.dot(returned, out_lat, preferred_element_type=jnp.float32)
    normed_mlp = normalize(second, norm_mlp)
    gate = jnp.dot(normed_mlp, w_gate, preferred_element_type=jnp.float32)
    upper = jnp.dot(normed_mlp, w_up, preferred_element_type=jnp.float32)
    hidden = (jax.nn.silu(gate) * upper).astype(jnp.bfloat16)
    return (second + jnp.dot(hidden, w_down, preferred_element_type=jnp.float32)).astype(
        jnp.bfloat16
    )


NT = (((1,), (1,)), ((), ()))
MESH = pl.DeviceIdType.MESH
F32 = jnp.float32
BF16 = jnp.bfloat16


def mm(a, b):
    return jnp.dot(a, b, preferred_element_type=F32)


def mm_nt(a, b):
    return lax.dot_general(a, b, NT, preferred_element_type=F32)


def iota(shape, dim):
    return lax.broadcasted_iota(jnp.int32, shape, dim)


def heads_t(keys, queries_t, values_t, temp, bias, table, mask, heads, size):
    outs = []
    for h in range(heads):
        part = slice(h * size, (h + 1) * size)
        scores = mm(keys[:, part], queries_t[part, :])
        scores = scores * (temp[:, h:h + 1] / math.sqrt(size)) + bias[:, h:h + 1] * table
        if mask is not None:
            scores = scores + mask
        expo = jnp.exp(scores - jnp.max(scores, axis=0, keepdims=True))
        denom = jnp.sum(expo, axis=0, keepdims=True)
        outs.append(mm(values_t[part, :], expo.astype(BF16)) / denom)
    return jnp.concatenate(outs, axis=0).astype(BF16)


def block_kernel(
    n_lon, n_lat, rows, width, depth, heads,
    fields_h, gain_lon_h, gain_lat_h, gain_mlp_h, temp_lon_h, bias_lon_h, temp_lat_h, bias_lat_h,
    wave_h, wq1_h, wk1_h, wv1_h, wo1_h, wq2_h, wk2_h, wv2_h, wo2_h, wg_h, wu_h, wd_h,
    out,
    fields, gain_lon, gain_lat, gain_mlp, temp_lon, bias_lon, temp_lat, bias_lat,
    wave, wq1, wk1, wv1, wo1, wq2, wk2, wv2, wo2, wg, wu, wd,
    norm_out, norm_in, field_out, field_in, att_out, att_in, upd_out,
    local_sem, s1, r1, s2, r2, s3, r3, s4, r4,
):
    me_lon = lax.axis_index("lon")
    me_lat = lax.axis_index("lat")
    total = n_lon * n_lat
    me = me_lon * n_lat + me_lat
    size = depth // heads
    cols = width // n_lat
    count = n_lat * rows
    cells = rows * width

    barrier = pltpu.get_barrier_semaphore()

    def greet(step, carry):
        peer = lax.rem(me + step, total)
        pl.semaphore_signal(
            barrier, inc=1, device_id=(peer // n_lat, lax.rem(peer, n_lat)), device_id_type=MESH
        )
        return carry

    lax.fori_loop(1, total, greet, 0)

    loads = [
        pltpu.make_async_copy(src, dst, local_sem.at[i])
        for i, (src, dst) in enumerate(
            [(fields_h, fields), (gain_lon_h, gain_lon), (wq1_h, wq1), (wk1_h, wk1), (wv1_h, wv1), (wave_h, wave), (wo1_h, wo1), (wq2_h, wq2),
             (wk2_h, wk2), (wv2_h, wv2), (wo2_h, wo2), (wg_h, wg), (wu_h, wu), (wd_h, wd),
             (gain_lat_h, gain_lat), (gain_mlp_h, gain_mlp), (temp_lon_h, temp_lon), (bias_lon_h, bias_lon),
             (temp_lat_h, temp_lat), (bias_lat_h, bias_lat)]
        )
    ]
    for load in loads:
        load.start()

    for load in loads[:2]:
        load.wait()
    wide = fields[...].astype(F32)
    norm_out[...] = normalize(wide, gain_lon[...][None])
    pieces = wide.reshape(rows, n_lat, cols, depth).astype(BF16)
    for a in range(n_lat):
        field_out[a] = pieces[:, a]

    pl.semaphore_wait(barrier, total - 1)

    def send_norm(step):
        peer = lax.rem(me_lon + step, n_lon)
        return pltpu.make_async_remote_copy(
            src_ref=norm_out.at[peer], dst_ref=norm_in.at[me_lon], send_sem=s1.at[step],
            recv_sem=r1.at[step], device_id=(peer, me_lat), device_id_type=MESH,
        )

    def lat_copy(step, src, dst, ssem, rsem):
        peer = lax.rem(me_lat + step, n_lat)
        return pltpu.make_async_remote_copy(
            src_ref=src.at[peer], dst_ref=dst.at[me_lat], send_sem=ssem.at[step],
            recv_sem=rsem.at[step], device_id=(me_lon, peer), device_id_type=MESH,
        )

    sends1 = [send_norm(step) for step in range(1, n_lon)]
    for copy in sends1:
        copy.start()
    sends2 = [lat_copy(step, field_out, field_in, s2, r2) for step in range(1, n_lat)]
    for copy in sends2:
        copy.start()
    norm_in[pl.ds(me_lon, 1)] = norm_out[pl.ds(me_lon, 1)]
    field_in[pl.ds(me_lat, 1)] = field_out[pl.ds(me_lat, 1)]

    shape = (cells, cells)
    lanes = iota(shape, 1)
    subs = iota(shape, 0)
    to_cols = (lax.rem(subs, count) * cols + subs // count == lanes).astype(F32).astype(BF16)
    from_cols = (lax.rem(lanes, count) * cols + lanes // count == subs).astype(F32).astype(BF16)
    eye = (lanes == subs).astype(F32).astype(BF16)
    half = cells // 2
    hs, hl = iota((half, half), 0), iota((half, half), 1)
    spread = jnp.abs(lax.rem(hs, count) - lax.rem(hl, count)).astype(F32) / count
    mask = jnp.where(hs // count == hl // count, 0.0, -1e30).astype(F32)

    early = loads[2:6] + loads[16:18]
    for load in early:
        load.wait()
    wq_t = wq1[...].T
    wv_t = wv1[...].T

    for copy in sends1:
        copy.wait_recv()

    nlon = n_lon * width
    normed = norm_in[...].reshape(nlon, depth)
    keys = mm(normed, wk1[...]).astype(BF16)
    queries_t = mm_nt(wq_t, normed).astype(BF16)
    values_t = mm_nt(wv_t, normed).astype(BF16)
    my_row = me_lat * rows + me_lon

    def att_copy(peer, row):
        return pltpu.make_async_remote_copy(
            src_ref=att_out.at[peer], dst_ref=att_in.at[row], send_sem=s3.at[peer],
            recv_sem=r3.at[row], device_id=(peer // n_lat, lax.rem(peer, n_lat)),
            device_id_type=MESH,
        )

    batch = min(nlon, 128)
    group = batch // cols
    for start in range(0, nlon, batch):
        span = slice(start, start + batch)
        att_t = heads_t(keys, queries_t[:, span], values_t, temp_lon, bias_lon, wave[:, span], None, heads, size)
        att = mm_nt(eye[:batch, :batch], att_t)
        first_peer = start // cols
        att_out[first_peer:first_peer + group] = att.reshape(group, cols, depth).astype(BF16)

        def start_att(step, carry, first_peer=first_peer):
            peer = first_peer + lax.rem(me + step, group)

            @pl.when(peer != me)
            def _():
                att_copy(peer, my_row).start()

            return carry

        lax.fori_loop(0, group, start_att, 0)
    att_in[pl.ds(my_row, 1)] = att_out[pl.ds(me, 1)]

    def wait_att(step, carry):
        att_copy(lax.rem(me + step, total), lax.rem(my_row + step, count)).wait_recv()
        return carry

    def wait_att_send(step, carry):
        att_copy(lax.rem(me + step, total), my_row).wait_send()
        return carry

    for load in loads[6:16] + loads[18:]:
        load.wait()
    wq2_t = wq2[...].T
    wv2_t = wv2[...].T
    for copy in sends2:
        copy.wait_recv()
    lax.fori_loop(1, total, wait_att, 0)

    resid = field_in[...].astype(F32).reshape(cells, depth)
    attended = att_in[...].astype(F32).reshape(cells, depth).astype(BF16)
    first = resid + mm(attended, wo1[...])
    normed = mm(to_cols, normalize(first, gain_lat[...])).astype(BF16)
    keys = mm(normed, wk2[...]).astype(BF16)
    queries_t = mm_nt(wq2_t, normed).astype(BF16)
    values_t = mm_nt(wv2_t, normed).astype(BF16)
    parts = []
    for part in (slice(0, half), slice(half, cells)):
        parts.append(
            heads_t(keys[part], queries_t[:, part], values_t[:, part], temp_lat, bias_lat,
                    spread, mask, heads, size)
        )
    att_t = jnp.concatenate(parts, axis=1)
    attended = mm_nt(from_cols, att_t).astype(BF16)
    second = first + mm(attended, wo2[...])
    normed = normalize(second, gain_mlp[...])
    ff = wg.shape[1]
    step_ff = min(ff, 256)
    for f in range(0, ff, step_ff):
        gate = mm(normed, wg[:, f:f + step_ff])
        upper = mm(normed, wu[:, f:f + step_ff])
        hidden = (gate / (1.0 + jnp.exp(-gate)) * upper).astype(BF16)
        second = second + mm(hidden, wd[f:f + step_ff, :])
    upd_out[...] = second.reshape(n_lat, rows, cols, depth).astype(BF16)

    def upd_copy(step):
        peer = lax.rem(me_lat + step, n_lat)
        return pltpu.make_async_remote_copy(
            src_ref=upd_out.at[peer], dst_ref=out.at[:, pl.ds(pl.multiple_of(me_lat * cols, cols), cols), :],
            send_sem=s4.at[step], recv_sem=r4.at[step], device_id=(me_lon, peer), device_id_type=MESH,
        )

    sends4 = [upd_copy(step) for step in range(1, n_lat)]
    for copy in sends4:
        copy.start()
    own = pltpu.make_async_copy(
        upd_out.at[me_lat], out.at[:, pl.ds(pl.multiple_of(me_lat * cols, cols), cols), :], s4.at[0]
    )
    own.start()
    for copy in sends1:
        copy.wait_send()
    for copy in sends2:
        copy.wait_send()
    lax.fori_loop(1, total, wait_att_send, 0)
    own.wait()
    for copy in sends4:
        copy.wait()


def fused_body(
    fields, norm_lon, query_lon, key_lon, value_lon, out_lon, temp_lon, bias_lon,
    norm_lat, query_lat, key_lat, value_lat, out_lat, temp_lat, bias_lat,
    norm_mlp, w_gate, w_up, w_down,
):
    rows, width, depth = fields.shape
    heads = temp_lon.shape[0]
    n_lon, n_lat = lax.axis_size("lon"), lax.axis_size("lat")
    cols = width // n_lat
    nlon = width * n_lon
    total = n_lon * n_lat
    place = np.arange(nlon)
    wave = np.cos((place[:, None] - place[None, :]) * (2.0 * math.pi / nlon)).astype(np.float32)
    hbm = pl.BlockSpec(memory_space=pl.ANY)
    weights = (query_lon, key_lon, value_lon, out_lon, query_lat, key_lat, value_lat, out_lat,
               w_gate, w_up, w_down)
    dma = pltpu.SemaphoreType.DMA
    updated = pl.pallas_call(
        functools.partial(block_kernel, n_lon, n_lat, rows, width, depth, heads),
        out_shape=jax.ShapeDtypeStruct((rows, width, depth), BF16),
        in_specs=[hbm] * 20,
        out_specs=hbm,
        scratch_shapes=[pltpu.VMEM((rows, width, depth), BF16)]
        + [pltpu.VMEM((1, depth), F32)] * 3
        + [pltpu.VMEM((1, heads), F32)] * 4
        + [pltpu.VMEM((nlon, nlon), F32)]
        + [pltpu.VMEM(w.shape, w.dtype) for w in weights]
        + [
            pltpu.VMEM((rows, width, depth), BF16),
            pltpu.VMEM((n_lon, width, depth), BF16),
            pltpu.VMEM((n_lat, rows, cols, depth), BF16),
            pltpu.VMEM((n_lat, rows, cols, depth), BF16),
            pltpu.VMEM((total, cols, depth), BF16),
            pltpu.VMEM((n_lat * rows, cols, depth), BF16),
            pltpu.VMEM((n_lat, rows, cols, depth), BF16),
            dma((20,)),
            dma((n_lon,)), dma((n_lon,)),
            dma((n_lat,)), dma((n_lat,)),
            dma((total,)), dma((total,)),
            dma((n_lat,)), dma((n_lat,)),
        ],
        compiler_params=pltpu.CompilerParams(collective_id=0, has_side_effects=True),
    )(
        fields, norm_lon[None], norm_lat[None], norm_mlp[None], temp_lon[None], bias_lon[None],
        temp_lat[None], bias_lat[None],
        jnp.asarray(wave), *weights,
    )
    return updated


def choose(*args):
    rows, width, _ = args[0].shape
    n_lon, n_lat = lax.axis_size("lon"), lax.axis_size("lat")
    if rows == n_lon and width % n_lat == 0 and width // n_lat == 8:
        return fused_body(*args)
    return body(*args)


def solution(mesh):
    in_specs = (P("lat", "lon", None),) + (P(),) * 18
    out_specs = P("lat", "lon", None)
    return jax.shard_map(choose, mesh=mesh, in_specs=in_specs, out_specs=out_specs, check_vma=False)
```

```python
import math

import jax
import jax.numpy as jnp
import functools
import numpy as np
from jax import lax
from jax.experimental import pallas as pl
from jax.experimental.pallas import tpu as pltpu
from jax.sharding import PartitionSpec as P


def normalize(values, gain):
    factor = lax.rsqrt(jnp.mean(values * values, axis=-1, keepdims=True) + 1e-06)
    return (values * factor * gain).astype(jnp.bfloat16)


def project(values, weight):
    return jnp.dot(values, weight, preferred_element_type=jnp.float32).astype(jnp.bfloat16)


def attend_lat(queries, keys, values, temp, bias):
    count, cols, depth = queries.shape
    heads = temp.shape[0]
    size = depth // heads
    qh = queries.reshape(count, cols, heads, size)
    kh = keys.reshape(count, cols, heads, size)
    vh = values.reshape(count, cols, heads, size)
    scores = jnp.einsum("ichd,jchd->chij", qh, kh, preferred_element_type=jnp.float32)
    place = jnp.arange(count, dtype=jnp.int32)
    spread = jnp.abs(place[:, None] - place[None, :]).astype(jnp.float32) / count
    scores = (
        scores * (temp / math.sqrt(size))[None, :, None, None]
        + bias[None, :, None, None] * spread[None, None]
    )
    expo = jnp.exp(scores - jnp.max(scores, axis=-1, keepdims=True))
    denom = jnp.sum(expo, axis=-1)
    mixed = jnp.einsum(
        "chij,jchd->ichd", expo.astype(jnp.bfloat16), vh, preferred_element_type=jnp.float32
    )
    mixed = mixed / jnp.transpose(denom, (2, 0, 1))[..., None]
    return mixed.astype(jnp.bfloat16).reshape(count, cols, depth)


def body(
    fields,
    norm_lon,
    query_lon,
    key_lon,
    value_lon,
    out_lon,
    temp_lon,
    bias_lon,
    norm_lat,
    query_lat,
    key_lat,
    value_lat,
    out_lat,
    temp_lat,
    bias_lat,
    norm_mlp,
    w_gate,
    w_up,
    w_down,
):
    rows, width, depth = fields.shape
    heads = temp_lon.shape[0]
    size = depth // heads
    total_lon = width * lax.axis_size("lon")
    resid = fields.astype(jnp.float32)
    normed = normalize(resid, norm_lon)
    scale_lon = temp_lon / math.sqrt(size)
    query_place = lax.axis_index("lon") * width + jnp.arange(width, dtype=jnp.int32)
    queries = project(normed, query_lon).reshape(rows, width, heads, size)
    piece = lax.all_gather(normed, "lon", axis=1, tiled=True)
    keys = project(piece, key_lon)
    count = keys.shape[1]
    key_place = jnp.arange(count, dtype=jnp.int32)
    angle = (query_place[:, None] - key_place[None, :]).astype(jnp.float32) * (
        2.0 * math.pi / total_lon
    )
    wave = jnp.cos(angle)

    def one_row(items):
        query_row, key_row, value_row, peak, total, accum = items
        key_heads = key_row.reshape(count, heads, size)
        value_heads = value_row.reshape(count, heads, size)
        scores = jnp.einsum(
            "ihd,jhd->hij", query_row, key_heads, preferred_element_type=jnp.float32
        )
        scores = scores * scale_lon[:, None, None] + bias_lon[:, None, None] * wave[None]
        fresh = jnp.maximum(peak, jnp.max(scores, axis=-1))
        shrink = jnp.exp(peak - fresh)
        expo = jnp.exp(scores - fresh[..., None])
        total = total * shrink + jnp.sum(expo, axis=-1)
        mixed = jnp.einsum(
            "hij,jhd->ihd",
            expo.astype(jnp.bfloat16),
            value_heads,
            preferred_element_type=jnp.float32,
        )
        accum = accum.reshape(width, heads, size) * jnp.transpose(shrink)[:, :, None] + mixed
        return (fresh, total, accum.reshape(width, depth))

    peak = jnp.full((rows, heads, width), -1e30, jnp.float32)
    total = jnp.zeros((rows, heads, width), jnp.float32)
    accum = jnp.zeros((rows, width, depth), jnp.float32)
    peak, total, accum = lax.map(
        one_row, (queries, keys, project(piece, value_lon), peak, total, accum)
    )
    attended = accum.reshape(rows, width, heads, size) / jnp.transpose(total, (0, 2, 1))[..., None]
    attended = attended.astype(jnp.bfloat16).reshape(rows, width, depth)
    first = resid + jnp.dot(attended, out_lon, preferred_element_type=jnp.float32)
    normed_lat = normalize(first, norm_lat)
    query_col = project(normed_lat, query_lat)
    key_col = project(normed_lat, key_lat)
    value_col = project(normed_lat, value_lat)
    query_col, key_col, value_col = (
        lax.all_to_all(query_col, "lat", split_axis=1, concat_axis=0, tiled=True),
        lax.all_to_all(key_col, "lat", split_axis=1, concat_axis=0, tiled=True),
        lax.all_to_all(value_col, "lat", split_axis=1, concat_axis=0, tiled=True),
    )
    mixed_lat = attend_lat(query_col, key_col, value_col, temp_lat, bias_lat)
    returned = lax.all_to_all(mixed_lat, "lat", split_axis=0, concat_axis=1, tiled=True)
    second = first + jnp.dot(returned, out_lat, preferred_element_type=jnp.float32)
    normed_mlp = normalize(second, norm_mlp)
    gate = jnp.dot(normed_mlp, w_gate, preferred_element_type=jnp.float32)
    upper = jnp.dot(normed_mlp, w_up, preferred_element_type=jnp.float32)
    hidden = (jax.nn.silu(gate) * upper).astype(jnp.bfloat16)
    return (second + jnp.dot(hidden, w_down, preferred_element_type=jnp.float32)).astype(
        jnp.bfloat16
    )


NT = (((1,), (1,)), ((), ()))
MESH = pl.DeviceIdType.MESH
F32 = jnp.float32
BF16 = jnp.bfloat16


def mm(a, b):
    return jnp.dot(a, b, preferred_element_type=F32)


def mm_nt(a, b):
    return lax.dot_general(a, b, NT, preferred_element_type=F32)


def iota(shape, dim):
    return lax.broadcasted_iota(jnp.int32, shape, dim)


def heads_t(keys, queries_t, values_t, temp, bias, table, mask, heads, size):
    outs = []
    for h in range(heads):
        part = slice(h * size, (h + 1) * size)
        scores = mm(keys[:, part], queries_t[part, :])
        scores = scores * (temp[:, h:h + 1] / math.sqrt(size)) + bias[:, h:h + 1] * table
        if mask is not None:
            scores = scores + mask
        expo = jnp.exp(scores - jnp.max(scores, axis=0, keepdims=True))
        denom = jnp.sum(expo, axis=0, keepdims=True)
        outs.append(mm(values_t[part, :], expo.astype(BF16)) / denom)
    return jnp.concatenate(outs, axis=0).astype(BF16)


def block_kernel(
    n_lon, n_lat, rows, width, depth, heads,
    fields_h, gain_lon_h, gain_lat_h, gain_mlp_h, temp_lon_h, bias_lon_h, temp_lat_h, bias_lat_h,
    wave_h, wq1_h, wk1_h, wv1_h, wo1_h, wq2_h, wk2_h, wv2_h, wo2_h, wg_h, wu_h, wd_h,
    out,
    fields, gain_lon, gain_lat, gain_mlp, temp_lon, bias_lon, temp_lat, bias_lat,
    wave, wq1, wk1, wv1, wo1, wq2, wk2, wv2, wo2, wg, wu, wd,
    norm_out, norm_in, field_out, field_in, att_out, att_in, upd_out,
    local_sem, s1, r1, s2, r2, s3, r3, s4, r4,
):
    me_lon = lax.axis_index("lon")
    me_lat = lax.axis_index("lat")
    total = n_lon * n_lat
    me = me_lon * n_lat + me_lat
    size = depth // heads
    cols = width // n_lat
    count = n_lat * rows
    cells = rows * width

    barrier = pltpu.get_barrier_semaphore()

    def greet(step, carry):
        peer = lax.rem(me + step, total)
        pl.semaphore_signal(
            barrier, inc=1, device_id=(peer // n_lat, lax.rem(peer, n_lat)), device_id_type=MESH
        )
        return carry

    lax.fori_loop(1, total, greet, 0)

    loads = [
        pltpu.make_async_copy(src, dst, local_sem.at[i])
        for i, (src, dst) in enumerate(
            [(fields_h, fields), (gain_lon_h, gain_lon), (wq1_h, wq1), (wk1_h, wk1), (wv1_h, wv1), (wave_h, wave), (wo1_h, wo1), (wq2_h, wq2),
             (wk2_h, wk2), (wv2_h, wv2), (wo2_h, wo2), (wg_h, wg), (wu_h, wu), (wd_h, wd),
             (gain_lat_h, gain_lat), (gain_mlp_h, gain_mlp), (temp_lon_h, temp_lon), (bias_lon_h, bias_lon),
             (temp_lat_h, temp_lat), (bias_lat_h, bias_lat)]
        )
    ]
    for load in loads:
        load.start()

    for load in loads[:2]:
        load.wait()
    wide = fields[...].astype(F32)
    norm_out[...] = normalize(wide, gain_lon[...][None])
    pieces = wide.reshape(rows, n_lat, cols, depth).astype(BF16)
    for a in range(n_lat):
        field_out[a] = pieces[:, a]

    pl.semaphore_wait(barrier, total - 1)

    def send_norm(step):
        peer = lax.rem(me_lon + step, n_lon)
        return pltpu.make_async_remote_copy(
            src_ref=norm_out.at[peer], dst_ref=norm_in.at[me_lon], send_sem=s1.at[step],
            recv_sem=r1.at[step], device_id=(peer, me_lat), device_id_type=MESH,
        )

    def lat_copy(step, src, dst, ssem, rsem):
        peer = lax.rem(me_lat + step, n_lat)
        return pltpu.make_async_remote_copy(
            src_ref=src.at[peer], dst_ref=dst.at[me_lat], send_sem=ssem.at[step],
            recv_sem=rsem.at[step], device_id=(me_lon, peer), device_id_type=MESH,
        )

    sends1 = [send_norm(step) for step in range(1, n_lon)]
    for copy in sends1:
        copy.start()
    sends2 = [lat_copy(step, field_out, field_in, s2, r2) for step in range(1, n_lat)]
    for copy in sends2:
        copy.start()
    norm_in[pl.ds(me_lon, 1)] = norm_out[pl.ds(me_lon, 1)]
    field_in[pl.ds(me_lat, 1)] = field_out[pl.ds(me_lat, 1)]

    shape = (cells, cells)
    lanes = iota(shape, 1)
    subs = iota(shape, 0)
    to_cols = (lax.rem(subs, count) * cols + subs // count == lanes).astype(F32).astype(BF16)
    from_cols = (lax.rem(lanes, count) * cols + lanes // count == subs).astype(F32).astype(BF16)
    eye = (lanes == subs).astype(F32).astype(BF16)
    half = cells // 2
    hs, hl = iota((half, half), 0), iota((half, half), 1)
    spread = jnp.abs(lax.rem(hs, count) - lax.rem(hl, count)).astype(F32) / count
    mask = jnp.where(hs // count == hl // count, 0.0, -1e30).astype(F32)

    early = loads[2:6] + loads[16:18]
    for load in early:
        load.wait()
    wq_t = wq1[...].T
    wv_t = wv1[...].T

    for copy in sends1:
        copy.wait_recv()

    nlon = n_lon * width
    normed = norm_in[...].reshape(nlon, depth)
    keys = mm(normed, wk1[...]).astype(BF16)
    queries_t = mm_nt(wq_t, normed).astype(BF16)
    values_t = mm_nt(wv_t, normed).astype(BF16)
    my_row = me_lat * rows + me_lon

    def att_copy(peer, row):
        return pltpu.make_async_remote_copy(
            src_ref=att_out.at[peer], dst_ref=att_in.at[row], send_sem=s3.at[peer],
            recv_sem=r3.at[row], device_id=(peer // n_lat, lax.rem(peer, n_lat)),
            device_id_type=MESH,
        )

    batch = min(nlon, 128)
    group = batch // cols
    for start in range(0, nlon, batch):
        span = slice(start, start + batch)
        att_t = heads_t(keys, queries_t[:, span], values_t, temp_lon, bias_lon, wave[:, span], None, heads, size)
        att = mm_nt(eye[:batch, :batch], att_t)
        first_peer = start // cols
        att_out[first_peer:first_peer + group] = att.reshape(group, cols, depth).astype(BF16)

        def start_att(step, carry, first_peer=first_peer):
            peer = first_peer + lax.rem(me + step, group)

            @pl.when(peer != me)
            def _():
                att_copy(peer, my_row).start()

            return carry

        lax.fori_loop(0, group, start_att, 0)
    att_in[pl.ds(my_row, 1)] = att_out[pl.ds(me, 1)]

    def wait_att(step, carry):
        att_copy(lax.rem(me + step, total), lax.rem(my_row + step, count)).wait_recv()
        return carry

    def wait_att_send(step, carry):
        att_copy(lax.rem(me + step, total), my_row).wait_send()
        return carry

    for load in loads[6:16] + loads[18:]:
        load.wait()
    wq2_t = wq2[...].T
    wv2_t = wv2[...].T
    for copy in sends2:
        copy.wait_recv()
    lax.fori_loop(1, total, wait_att, 0)

    resid = field_in[...].astype(F32).reshape(cells, depth)
    attended = att_in[...].astype(F32).reshape(cells, depth).astype(BF16)
    first = resid + mm(attended, wo1[...])
    normed = mm(to_cols, normalize(first, gain_lat[...])).astype(BF16)
    keys = mm(normed, wk2[...]).astype(BF16)
    queries_t = mm_nt(wq2_t, normed).astype(BF16)
    values_t = mm_nt(wv2_t, normed).astype(BF16)
    parts = []
    for part in (slice(0, half), slice(half, cells)):
        parts.append(
            heads_t(keys[part], queries_t[:, part], values_t[:, part], temp_lat, bias_lat,
                    spread, mask, heads, size)
        )
    att_t = jnp.concatenate(parts, axis=1)
    attended = mm_nt(from_cols, att_t).astype(BF16)
    second = first + mm(attended, wo2[...])
    normed = normalize(second, gain_mlp[...])
    ff = wg.shape[1]
    step_ff = min(ff, 256)
    for f in range(0, ff, step_ff):
        gate = mm(normed, wg[:, f:f + step_ff])
        upper = mm(normed, wu[:, f:f + step_ff])
        hidden = (gate / (1.0 + jnp.exp(-gate)) * upper).astype(BF16)
        second = second + mm(hidden, wd[f:f + step_ff, :])
    upd_out[...] = second.reshape(n_lat, rows, cols, depth).astype(BF16)

    def upd_copy(step):
        peer = lax.rem(me_lat + step, n_lat)
        return pltpu.make_async_remote_copy(
            src_ref=upd_out.at[peer], dst_ref=out.at[:, pl.ds(pl.multiple_of(me_lat * cols, cols), cols), :],
            send_sem=s4.at[step], recv_sem=r4.at[step], device_id=(me_lon, peer), device_id_type=MESH,
        )

    sends4 = [upd_copy(step) for step in range(1, n_lat)]
    for copy in sends4:
        copy.start()
    own = pltpu.make_async_copy(
        upd_out.at[me_lat], out.at[:, pl.ds(pl.multiple_of(me_lat * cols, cols), cols), :], s4.at[0]
    )
    own.start()
    for copy in sends1:
        copy.wait_send()
    for copy in sends2:
        copy.wait_send()
    lax.fori_loop(1, total, wait_att_send, 0)
    own.wait()
    for copy in sends4:
        copy.wait()


def fused_body(
    fields, norm_lon, query_lon, key_lon, value_lon, out_lon, temp_lon, bias_lon,
    norm_lat, query_lat, key_lat, value_lat, out_lat, temp_lat, bias_lat,
    norm_mlp, w_gate, w_up, w_down,
):
    rows, width, depth = fields.shape
    heads = temp_lon.shape[0]
    n_lon, n_lat = lax.axis_size("lon"), lax.axis_size("lat")
    cols = width // n_lat
    nlon = width * n_lon
    total = n_lon * n_lat
    place = np.arange(nlon)
    wave = np.cos((place[:, None] - place[None, :]) * (2.0 * math.pi / nlon)).astype(np.float32)
    hbm = pl.BlockSpec(memory_space=pl.ANY)
    weights = (query_lon, key_lon, value_lon, out_lon, query_lat, key_lat, value_lat, out_lat,
               w_gate, w_up, w_down)
    dma = pltpu.SemaphoreType.DMA
    updated = pl.pallas_call(
        functools.partial(block_kernel, n_lon, n_lat, rows, width, depth, heads),
        out_shape=pltpu.VMEM((rows, width, depth), BF16),
        in_specs=[hbm] * 20,
        out_specs=hbm,
        scratch_shapes=[pltpu.VMEM((rows, width, depth), BF16)]
        + [pltpu.VMEM((1, depth), F32)] * 3
        + [pltpu.VMEM((1, heads), F32)] * 4
        + [pltpu.VMEM((nlon, nlon), F32)]
        + [pltpu.VMEM(w.shape, w.dtype) for w in weights]
        + [
            pltpu.VMEM((rows, width, depth), BF16),
            pltpu.VMEM((n_lon, width, depth), BF16),
            pltpu.VMEM((n_lat, rows, cols, depth), BF16),
            pltpu.VMEM((n_lat, rows, cols, depth), BF16),
            pltpu.VMEM((total, cols, depth), BF16),
            pltpu.VMEM((n_lat * rows, cols, depth), BF16),
            pltpu.VMEM((n_lat, rows, cols, depth), BF16),
            dma((20,)),
            dma((n_lon,)), dma((n_lon,)),
            dma((n_lat,)), dma((n_lat,)),
            dma((total,)), dma((total,)),
            dma((n_lat,)), dma((n_lat,)),
        ],
        compiler_params=pltpu.CompilerParams(collective_id=0, has_side_effects=True),
    )(
        fields, norm_lon[None], norm_lat[None], norm_mlp[None], temp_lon[None], bias_lon[None],
        temp_lat[None], bias_lat[None],
        jnp.asarray(wave), *weights,
    )
    return updated


def choose(*args):
    rows, width, _ = args[0].shape
    n_lon, n_lat = lax.axis_size("lon"), lax.axis_size("lat")
    if rows == n_lon and width % n_lat == 0 and width // n_lat == 8:
        return fused_body(*args)
    return body(*args)


def solution(mesh):
    in_specs = (P("lat", "lon", None),) + (P(),) * 18
    out_specs = P("lat", "lon", None)
    return jax.shard_map(choose, mesh=mesh, in_specs=in_specs, out_specs=out_specs, check_vma=False)
```

```python
import math

import jax
import jax.numpy as jnp
import functools
import numpy as np
from jax import lax
from jax.experimental import pallas as pl
from jax.experimental.pallas import tpu as pltpu
from jax.sharding import PartitionSpec as P


def normalize(values, gain):
    factor = lax.rsqrt(jnp.mean(values * values, axis=-1, keepdims=True) + 1e-06)
    return (values * factor * gain).astype(jnp.bfloat16)


def project(values, weight):
    return jnp.dot(values, weight, preferred_element_type=jnp.float32).astype(jnp.bfloat16)


def attend_lat(queries, keys, values, temp, bias):
    count, cols, depth = queries.shape
    heads = temp.shape[0]
    size = depth // heads
    qh = queries.reshape(count, cols, heads, size)
    kh = keys.reshape(count, cols, heads, size)
    vh = values.reshape(count, cols, heads, size)
    scores = jnp.einsum("ichd,jchd->chij", qh, kh, preferred_element_type=jnp.float32)
    place = jnp.arange(count, dtype=jnp.int32)
    spread = jnp.abs(place[:, None] - place[None, :]).astype(jnp.float32) / count
    scores = (
        scores * (temp / math.sqrt(size))[None, :, None, None]
        + bias[None, :, None, None] * spread[None, None]
    )
    expo = jnp.exp(scores - jnp.max(scores, axis=-1, keepdims=True))
    denom = jnp.sum(expo, axis=-1)
    mixed = jnp.einsum(
        "chij,jchd->ichd", expo.astype(jnp.bfloat16), vh, preferred_element_type=jnp.float32
    )
    mixed = mixed / jnp.transpose(denom, (2, 0, 1))[..., None]
    return mixed.astype(jnp.bfloat16).reshape(count, cols, depth)


def body(
    fields,
    norm_lon,
    query_lon,
    key_lon,
    value_lon,
    out_lon,
    temp_lon,
    bias_lon,
    norm_lat,
    query_lat,
    key_lat,
    value_lat,
    out_lat,
    temp_lat,
    bias_lat,
    norm_mlp,
    w_gate,
    w_up,
    w_down,
):
    rows, width, depth = fields.shape
    heads = temp_lon.shape[0]
    size = depth // heads
    total_lon = width * lax.axis_size("lon")
    resid = fields.astype(jnp.float32)
    normed = normalize(resid, norm_lon)
    scale_lon = temp_lon / math.sqrt(size)
    query_place = lax.axis_index("lon") * width + jnp.arange(width, dtype=jnp.int32)
    queries = project(normed, query_lon).reshape(rows, width, heads, size)
    piece = lax.all_gather(normed, "lon", axis=1, tiled=True)
    keys = project(piece, key_lon)
    count = keys.shape[1]
    key_place = jnp.arange(count, dtype=jnp.int32)
    angle = (query_place[:, None] - key_place[None, :]).astype(jnp.float32) * (
        2.0 * math.pi / total_lon
    )
    wave = jnp.cos(angle)

    def one_row(items):
        query_row, key_row, value_row, peak, total, accum = items
        key_heads = key_row.reshape(count, heads, size)
        value_heads = value_row.reshape(count, heads, size)
        scores = jnp.einsum(
            "ihd,jhd->hij", query_row, key_heads, preferred_element_type=jnp.float32
        )
        scores = scores * scale_lon[:, None, None] + bias_lon[:, None, None] * wave[None]
        fresh = jnp.maximum(peak, jnp.max(scores, axis=-1))
        shrink = jnp.exp(peak - fresh)
        expo = jnp.exp(scores - fresh[..., None])
        total = total * shrink + jnp.sum(expo, axis=-1)
        mixed = jnp.einsum(
            "hij,jhd->ihd",
            expo.astype(jnp.bfloat16),
            value_heads,
            preferred_element_type=jnp.float32,
        )
        accum = accum.reshape(width, heads, size) * jnp.transpose(shrink)[:, :, None] + mixed
        return (fresh, total, accum.reshape(width, depth))

    peak = jnp.full((rows, heads, width), -1e30, jnp.float32)
    total = jnp.zeros((rows, heads, width), jnp.float32)
    accum = jnp.zeros((rows, width, depth), jnp.float32)
    peak, total, accum = lax.map(
        one_row, (queries, keys, project(piece, value_lon), peak, total, accum)
    )
    attended = accum.reshape(rows, width, heads, size) / jnp.transpose(total, (0, 2, 1))[..., None]
    attended = attended.astype(jnp.bfloat16).reshape(rows, width, depth)
    first = resid + jnp.dot(attended, out_lon, preferred_element_type=jnp.float32)
    normed_lat = normalize(first, norm_lat)
    query_col = project(normed_lat, query_lat)
    key_col = project(normed_lat, key_lat)
    value_col = project(normed_lat, value_lat)
    query_col, key_col, value_col = (
        lax.all_to_all(query_col, "lat", split_axis=1, concat_axis=0, tiled=True),
        lax.all_to_all(key_col, "lat", split_axis=1, concat_axis=0, tiled=True),
        lax.all_to_all(value_col, "lat", split_axis=1, concat_axis=0, tiled=True),
    )
    mixed_lat = attend_lat(query_col, key_col, value_col, temp_lat, bias_lat)
    returned = lax.all_to_all(mixed_lat, "lat", split_axis=0, concat_axis=1, tiled=True)
    second = first + jnp.dot(returned, out_lat, preferred_element_type=jnp.float32)
    normed_mlp = normalize(second, norm_mlp)
    gate = jnp.dot(normed_mlp, w_gate, preferred_element_type=jnp.float32)
    upper = jnp.dot(normed_mlp, w_up, preferred_element_type=jnp.float32)
    hidden = (jax.nn.silu(gate) * upper).astype(jnp.bfloat16)
    return (second + jnp.dot(hidden, w_down, preferred_element_type=jnp.float32)).astype(
        jnp.bfloat16
    )


NT = (((1,), (1,)), ((), ()))
MESH = pl.DeviceIdType.MESH
F32 = jnp.float32
BF16 = jnp.bfloat16


def mm(a, b):
    return jnp.dot(a, b, preferred_element_type=F32)


def mm_nt(a, b):
    return lax.dot_general(a, b, NT, preferred_element_type=F32)


def iota(shape, dim):
    return lax.broadcasted_iota(jnp.int32, shape, dim)


def heads_t(keys, queries_t, values_t, temp, bias, table, mask, heads, size):
    outs = []
    for h in range(heads):
        part = slice(h * size, (h + 1) * size)
        scores = mm(keys[:, part], queries_t[part, :])
        scores = scores * (temp[:, h:h + 1] / math.sqrt(size)) + bias[:, h:h + 1] * table
        if mask is not None:
            scores = scores + mask
        expo = jnp.exp(scores - jnp.max(scores, axis=0, keepdims=True))
        denom = jnp.sum(expo, axis=0, keepdims=True)
        outs.append(mm(values_t[part, :], expo.astype(BF16)) / denom)
    return jnp.concatenate(outs, axis=0).astype(BF16)


def block_kernel(
    n_lon, n_lat, rows, width, depth, heads,
    fields_h, gain_lon_h, gain_lat_h, gain_mlp_h, temp_lon_h, bias_lon_h, temp_lat_h, bias_lat_h,
    wave_h, wq1_h, wk1_h, wv1_h, wo1_h, wq2_h, wk2_h, wv2_h, wo2_h, wg_h, wu_h, wd_h,
    out,
    fields, gain_lon, gain_lat, gain_mlp, temp_lon, bias_lon, temp_lat, bias_lat,
    wave, wq1, wk1, wv1, wo1, wq2, wk2, wv2, wo2, wg, wu, wd,
    norm_out, norm_in, field_out, field_in, att_out, att_in, upd_out, query_s, first_s, mixed_s,
    local_sem, s1, r1, s2, r2, s3, r3, s4, r4,
):
    me_lon = lax.axis_index("lon")
    me_lat = lax.axis_index("lat")
    total = n_lon * n_lat
    me = me_lon * n_lat + me_lat
    size = depth // heads
    cols = width // n_lat
    count = n_lat * rows
    cells = rows * width

    barrier = pltpu.get_barrier_semaphore()

    def greet(step, carry):
        peer = lax.rem(me + step, total)
        pl.semaphore_signal(
            barrier, inc=1, device_id=(peer // n_lat, lax.rem(peer, n_lat)), device_id_type=MESH
        )
        return carry

    lax.fori_loop(1, total, greet, 0)

    loads = [
        pltpu.make_async_copy(src, dst, local_sem.at[i])
        for i, (src, dst) in enumerate(
            [(fields_h, fields), (gain_lon_h, gain_lon), (wq1_h, wq1), (wk1_h, wk1), (wv1_h, wv1), (wave_h, wave), (wo1_h, wo1), (wq2_h, wq2),
             (wk2_h, wk2), (wv2_h, wv2), (wo2_h, wo2), (wg_h, wg), (wu_h, wu), (wd_h, wd),
             (gain_lat_h, gain_lat), (gain_mlp_h, gain_mlp), (temp_lon_h, temp_lon), (bias_lon_h, bias_lon),
             (temp_lat_h, temp_lat), (bias_lat_h, bias_lat)]
        )
    ]
    for load in loads:
        load.start()

    for load in loads[:2]:
        load.wait()
    wide = fields[...].astype(F32)
    norm_out[...] = normalize(wide, gain_lon[...][None])
    pieces = wide.reshape(rows, n_lat, cols, depth).astype(BF16)
    for a in range(n_lat):
        field_out[a] = pieces[:, a]

    pl.semaphore_wait(barrier, total - 1)

    def send_norm(step):
        peer = lax.rem(me_lon + step, n_lon)
        return pltpu.make_async_remote_copy(
            src_ref=norm_out.at[peer], dst_ref=norm_in.at[me_lon], send_sem=s1.at[step],
            recv_sem=r1.at[step], device_id=(peer, me_lat), device_id_type=MESH,
        )

    def lat_copy(step, src, dst, ssem, rsem):
        peer = lax.rem(me_lat + step, n_lat)
        return pltpu.make_async_remote_copy(
            src_ref=src.at[peer], dst_ref=dst.at[me_lat], send_sem=ssem.at[step],
            recv_sem=rsem.at[step], device_id=(me_lon, peer), device_id_type=MESH,
        )

    sends1 = [send_norm(step) for step in range(1, n_lon)]
    for copy in sends1:
        copy.start()
    sends2 = [lat_copy(step, field_out, field_in, s2, r2) for step in range(1, n_lat)]
    for copy in sends2:
        copy.start()
    norm_in[pl.ds(me_lon, 1)] = norm_out[pl.ds(me_lon, 1)]
    field_in[pl.ds(me_lat, 1)] = field_out[pl.ds(me_lat, 1)]

    shape = (cells, cells)
    lanes = iota(shape, 1)
    subs = iota(shape, 0)
    to_cols = (lax.rem(subs, count) * cols + subs // count == lanes).astype(F32).astype(BF16)
    from_cols = (lax.rem(lanes, count) * cols + lanes // count == subs).astype(F32).astype(BF16)
    eye = (lanes == subs).astype(F32).astype(BF16)
    half = cells // 2
    hs, hl = iota((half, half), 0), iota((half, half), 1)
    spread = jnp.abs(lax.rem(hs, count) - lax.rem(hl, count)).astype(F32) / count
    mask = jnp.where(hs // count == hl // count, 0.0, -1e30).astype(F32)

    early = loads[2:6] + loads[16:18]
    for load in early:
        load.wait()
    wq_t = wq1[...].T
    wv_t = wv1[...].T

    for copy in sends1:
        copy.wait_recv()

    nlon = n_lon * width
    normed = norm_in[...].reshape(nlon, depth)
    keys = mm(normed, wk1[...]).astype(BF16)
    query_s[...] = mm_nt(wq_t, normed).astype(BF16)
    values_t = mm_nt(wv_t, normed).astype(BF16)
    my_row = me_lat * rows + me_lon

    def att_copy(peer, row):
        return pltpu.make_async_remote_copy(
            src_ref=att_out.at[peer], dst_ref=att_in.at[row], send_sem=s3.at[peer],
            recv_sem=r3.at[row], device_id=(peer // n_lat, lax.rem(peer, n_lat)),
            device_id_type=MESH,
        )

    batch = min(nlon, 128)
    group = batch // cols
    lons = group // n_lat
    high = (2 * me_lat) // n_lat
    for turn in range(1, total // group + 1):
        part = lax.rem(me // group + turn, total // group)
        span = pl.ds(pl.multiple_of(part * batch, batch), batch)
        att_t = heads_t(keys, query_s[:, span], values_t, temp_lon, bias_lon, wave[:, span], None, heads, size)
        att = mm_nt(eye[:batch, :batch], att_t)
        att_out[pl.ds(part * group, group)] = att.reshape(group, cols, depth).astype(BF16)

        def start_att(step, carry, part=part):
            away = step // lons
            lat_peer = away + (1 - high) * (n_lat - 1 - 2 * away)
            peer = (part * lons + lax.rem(me_lon + step, lons)) * n_lat + lat_peer

            @pl.when(peer != me)
            def _():
                att_copy(peer, my_row).start()

            return carry

        lax.fori_loop(0, group, start_att, 0)
    att_in[pl.ds(my_row, 1)] = att_out[pl.ds(me, 1)]

    def wait_att(step, carry):
        att_copy(lax.rem(me + step, total), lax.rem(my_row + step, count)).wait_recv()
        return carry

    def wait_att_send(step, carry):
        att_copy(lax.rem(me + step, total), my_row).wait_send()
        return carry

    for load in loads[6:16] + loads[18:]:
        load.wait()
    wq2_t = wq2[...].T
    wv2_t = wv2[...].T
    for copy in sends2:
        copy.wait_recv()
    lax.fori_loop(1, total, wait_att, 0)

    resid = field_in[...].astype(F32).reshape(cells, depth)
    attended = att_in[...].astype(F32).reshape(cells, depth).astype(BF16)
    first = resid + mm(attended, wo1[...])
    normed = mm(to_cols, normalize(first, gain_lat[...])).astype(BF16)
    keys = mm(normed, wk2[...]).astype(BF16)
    queries_t = mm_nt(wq2_t, normed).astype(BF16)
    values_t = mm_nt(wv2_t, normed).astype(BF16)
    parts = []
    for part in (slice(0, half), slice(half, cells)):
        parts.append(
            heads_t(keys[part], queries_t[:, part], values_t[:, part], temp_lat, bias_lat,
                    spread, mask, heads, size)
        )
    att_t = jnp.concatenate(parts, axis=1)
    mixed_s[...] = mm_nt(from_cols, att_t).astype(BF16)
    first_s[...] = first

    def upd_copy(peer, owner):
        return pltpu.make_async_remote_copy(
            src_ref=upd_out.at[peer], dst_ref=out.at[:, pl.ds(pl.multiple_of(me_lat * cols, cols), cols), :],
            send_sem=s4.at[peer], recv_sem=r4.at[owner], device_id=(me_lon, peer), device_id_type=MESH,
        )

    ff = wg.shape[1]
    step_ff = min(ff, 256)
    near = n_lat // 2
    for turn in range(1, 3):
        part = lax.rem(high + turn, 2)
        span = pl.ds(pl.multiple_of(part * half, half), half)
        second = first_s[span, :] + mm(mixed_s[span, :], wo2[...])
        normed = normalize(second, gain_mlp[...])
        for f in range(0, ff, step_ff):
            gate = mm(normed, wg[:, f:f + step_ff])
            upper = mm(normed, wu[:, f:f + step_ff])
            hidden = (gate / (1.0 + jnp.exp(-gate)) * upper).astype(BF16)
            second = second + mm(hidden, wd[f:f + step_ff, :])
        upd_out[pl.ds(part * near, near)] = second.reshape(near, rows, cols, depth).astype(BF16)
        for away in range(near):
            peer = part * near + away + (1 - high) * (near - 1 - 2 * away)

            @pl.when(peer != me_lat)
            def _(peer=peer):
                upd_copy(peer, me_lat).start()

    own = pltpu.make_async_copy(
        upd_out.at[me_lat], out.at[:, pl.ds(pl.multiple_of(me_lat * cols, cols), cols), :], s4.at[me_lat]
    )
    own.start()
    for copy in sends1:
        copy.wait_send()
    for copy in sends2:
        copy.wait_send()
    lax.fori_loop(1, total, wait_att_send, 0)
    own.wait()
    for step in range(1, n_lat):
        peer = lax.rem(me_lat + step, n_lat)
        upd_copy(peer, peer).wait()


def fused_body(
    fields, norm_lon, query_lon, key_lon, value_lon, out_lon, temp_lon, bias_lon,
    norm_lat, query_lat, key_lat, value_lat, out_lat, temp_lat, bias_lat,
    norm_mlp, w_gate, w_up, w_down,
):
    rows, width, depth = fields.shape
    heads = temp_lon.shape[0]
    n_lon, n_lat = lax.axis_size("lon"), lax.axis_size("lat")
    cols = width // n_lat
    nlon = width * n_lon
    total = n_lon * n_lat
    place = np.arange(nlon)
    wave = np.cos((place[:, None] - place[None, :]) * (2.0 * math.pi / nlon)).astype(np.float32)
    hbm = pl.BlockSpec(memory_space=pl.ANY)
    weights = (query_lon, key_lon, value_lon, out_lon, query_lat, key_lat, value_lat, out_lat,
               w_gate, w_up, w_down)
    dma = pltpu.SemaphoreType.DMA
    updated = pl.pallas_call(
        functools.partial(block_kernel, n_lon, n_lat, rows, width, depth, heads),
        out_shape=pltpu.VMEM((rows, width, depth), BF16),
        in_specs=[hbm] * 20,
        out_specs=hbm,
        scratch_shapes=[pltpu.VMEM((rows, width, depth), BF16)]
        + [pltpu.VMEM((1, depth), F32)] * 3
        + [pltpu.VMEM((1, heads), F32)] * 4
        + [pltpu.VMEM((nlon, nlon), F32)]
        + [pltpu.VMEM(w.shape, w.dtype) for w in weights]
        + [
            pltpu.VMEM((rows, width, depth), BF16),
            pltpu.VMEM((n_lon, width, depth), BF16),
            pltpu.VMEM((n_lat, rows, cols, depth), BF16),
            pltpu.VMEM((n_lat, rows, cols, depth), BF16),
            pltpu.VMEM((total, cols, depth), BF16),
            pltpu.VMEM((n_lat * rows, cols, depth), BF16),
            pltpu.VMEM((n_lat, rows, cols, depth), BF16),
            pltpu.VMEM((depth, nlon), BF16),
            pltpu.VMEM((rows * width, depth), F32),
            pltpu.VMEM((rows * width, depth), BF16),
            dma((20,)),
            dma((n_lon,)), dma((n_lon,)),
            dma((n_lat,)), dma((n_lat,)),
            dma((total,)), dma((total,)),
            dma((n_lat,)), dma((n_lat,)),
        ],
        compiler_params=pltpu.CompilerParams(collective_id=0, has_side_effects=True),
    )(
        fields, norm_lon[None], norm_lat[None], norm_mlp[None], temp_lon[None], bias_lon[None],
        temp_lat[None], bias_lat[None],
        jnp.asarray(wave), *weights,
    )
    return updated


def choose(*args):
    rows, width, _ = args[0].shape
    n_lon, n_lat = lax.axis_size("lon"), lax.axis_size("lat")
    fits = rows == n_lon and width == 8 * n_lat and n_lat % 2 == 0 and 16 % n_lat == 0
    if fits and (width * n_lon) % 256 == 0:
        return fused_body(*args)
    return body(*args)


def solution(mesh):
    in_specs = (P("lat", "lon", None),) + (P(),) * 18
    out_specs = P("lat", "lon", None)
    return jax.shard_map(choose, mesh=mesh, in_specs=in_specs, out_specs=out_specs, check_vma=False)
```
